256 devices in a mesh: bank: 16 (over z, core), zero: 16 (over y, x).
Axes of the slice: x: 4, y: 4, z: 8, core: 2. Of those that a mesh axis runs over, the one named last changes fastest.
Arguments:
- master_down: float32 [64, 1024, 2048], P('bank', None, 'zero'), may hold values from -0.25 to 0.25
- second_down: bfloat16 [64, 1024, 2048], P('bank', None, 'zero'), may hold values from -0.09375 to 0.09375
- router_weight: float32 [2048, 64], P('zero', 'bank'), may hold values from -0.125 to 0.125
- router_gain: float32 [2048], P('zero'), may hold values from 0.25 to 1.75
Outputs:
- final_down: bfloat16 [64, 1024, 2048], P('bank')
- scale_down: float32 [64, 1024], P('bank')
- serve_router: bfloat16 [2048, 64], replicated
The draws below stay inside these ranges and needn't reach their ends.
All inputs are finite; a program needn't handle non-finite values. Where the reference program divides by a largest or mean magnitude, that divisor is 1e-20 or more.
Results may differ from the reference program's by a relative error of at most 0.001.
Values may be sent and summed in bfloat16 or wider, within the bound.
No kernel may reach another device: no remote copies, remote signals or barrier semaphores. Data moves between devices by JAX's collectives and lax.ppermute only.
A program may use at most 128 MiB of HBM per device.

```python
import jax
import jax.numpy as jnp

EXPERTS = 64
D_MODEL = 2048
D_EXPERT = 1024


def with_spikes(values, own_key, source, target, shards_of, factor):
    def block_of(position):
        return (jnp.arange(values.shape[position]) // (values.shape[position] // shards_of)).reshape((-1,) + (1,) * (values.ndim - 1 - position))

    near = jax.random.permutation(own_key, shards_of)[block_of(target)]
    second = (block_of(target) + shards_of // 2) % shards_of
    return jnp.where((block_of(source) == near) | (block_of(source) == second), factor * values, values)


def steps_of(stream_key, extent, cuts, least, top_value):
    factor_of, own = 1.0, jax.random.fold_in(stream_key, 6)
    for axis_at, parts in cuts:
        draws = jnp.exp(jax.random.uniform(jax.random.fold_in(own, axis_at), (parts,), jnp.float32, least / len(cuts), top_value / len(cuts)))
        factor_of = factor_of * jnp.repeat(draws, extent[axis_at] // parts).reshape([-1 if axis == axis_at else 1 for axis in range(len(extent))])
    return factor_of


def bell_draw(stream_key, shape, deviation, reach, split=(), dtype=jnp.bfloat16):
    factor_of = steps_of(stream_key, shape, split, -0.22, 0.18) if split else 1.0
    entries = jax.random.normal(stream_key, shape, jnp.float32) * deviation * factor_of
    return jnp.minimum(jnp.maximum(entries, -reach), reach).astype(dtype)


def noise_with(key, dims, width, bound, split, heavy, kind=jnp.bfloat16):
    entries = width * jax.random.normal(key, dims, jnp.float32)
    if split:
        entries = entries * steps_of(key, dims, split, -0.22, 0.18)
    return jnp.clip(with_spikes(entries, jax.random.fold_in(key, 3), *heavy), -bound, bound).astype(kind)


def setup_inputs(seed: int = 0) -> dict:
    key_of = jax.random.split(jax.random.key(seed), 5)
    master_down = noise_with(key_of[0], (EXPERTS, D_EXPERT, D_MODEL), D_EXPERT ** -0.5, 0.25, ((0, 16), (2, 16)), (2, 1, 16, 2.0), jnp.float32)
    second_down = bell_draw(key_of[1], (EXPERTS, D_EXPERT, D_MODEL), (D_EXPERT * 4) ** -0.5, 0.09375, ((0, 16), (2, 16)))
    router_weight = bell_draw(key_of[2], (D_MODEL, EXPERTS), D_MODEL ** -0.5, 0.125, ((0, 16), (1, 16)), jnp.float32)
    router_gain = jnp.clip(1.0 + 0.15 * jax.random.normal(key_of[3], (D_MODEL,), jnp.float32), 0.25, 1.75)
    return {"master_down": master_down, "second_down": second_down, "router_weight": router_weight, "router_gain": router_gain}


def reference(master_down, second_down, router_weight, router_gain):
    merged_down = master_down + second_down.astype(jnp.float32)
    scale_down = jnp.max(jnp.abs(merged_down), axis=2)
    final_down = (merged_down / jnp.expand_dims(scale_down, 2)).astype(jnp.bfloat16)
    serve_router = (router_weight * router_gain[:, None]).astype(jnp.bfloat16)
    return final_down, scale_down, serve_router
```

```python
import functools

import jax
import jax.numpy as jnp
from jax import lax
from jax.experimental import pallas as pl
from jax.experimental.pallas import tpu as pltpu
from jax.sharding import PartitionSpec as P

BANKS, ROWS, COLS = 16, 4, 4


def pairs(dy, dx):
    out = []
    for bank in range(BANKS):
        sign = 1 if bank % 2 == 0 else -1
        for y in range(ROWS):
            for x in range(COLS):
                to = ((y + sign * dy) % ROWS) * COLS + (x + sign * dx) % COLS
                out.append((bank * 16 + y * COLS + x, bank * 16 + to))
    return out


def hop(value, dy, dx):
    return lax.ppermute(value, ("bank", "zero"), pairs(dy, dx))


def from_everyone(value, axis):
    count = lax.axis_size(axis)
    return lax.all_to_all(jnp.broadcast_to(value[None], (count, *value.shape)), axis, 0, 0, tiled=True)


def place(at, blocks, out=None):
    arrays = [array for array, _ in blocks]
    n = sum(len(pieces) for _, pieces in blocks)

    def body(at_ref, *refs):
        out_ref, sems = refs[-2], refs[-1]
        copies = []
        for ref, (_, pieces) in zip(refs, blocks):
            for j, (expert, i) in enumerate(pieces):
                target = out_ref.at[pl.ds(expert, 2), :, pl.ds(pl.multiple_of(at_ref[i] * 128, 128), 128)]
                copies.append(pltpu.make_async_copy(ref.at[pl.ds(2 * j, 2)], target, sems.at[len(copies)]))
        for copy in copies:
            copy.start()
        for copy in copies:
            copy.wait()

    specs = [pl.BlockSpec(memory_space=pltpu.SMEM)] + [pl.BlockSpec(memory_space=pl.ANY)] * len(arrays)
    args = [at] + arrays
    aliases = {}
    if out is not None:
        aliases = {len(args): 0}
        specs.append(pl.BlockSpec(memory_space=pl.ANY))
        args.append(out)
    return pl.pallas_call(
        body,
        out_shape=jax.ShapeDtypeStruct((4, 1024, 2048), jnp.bfloat16),
        in_specs=specs,
        out_specs=pl.BlockSpec(memory_space=pl.ANY),
        scratch_shapes=[pltpu.SemaphoreType.DMA((n,))],
        input_output_aliases=aliases,
    )(*args)


def shards(master_down, second_down, router_weight, router_gain):
    merged = master_down + second_down.astype(jnp.float32)
    local = jnp.max(jnp.abs(merged), axis=2)
    part = (router_weight * router_gain[:, None]).T
    seen = from_everyone(jnp.concatenate([local, part], axis=1), "zero")
    scale_down = jnp.max(seen[:, :, :1024], axis=0)
    row = jnp.moveaxis(seen[:, :, 1024:], 0, 1).reshape(4, 2048).astype(jnp.bfloat16)
    narrow = (merged / jnp.expand_dims(scale_down, 2)).astype(jnp.bfloat16)

    step = {"a": ((0, 1), (1, 0)), "b": ((1, 0), (0, 1))}
    own = {"a": narrow[:2], "b": narrow[2:]}
    first = {c: [own[c]] for c in "ab"}
    for k in range(3):
        for c in "ab":
            first[c].append(hop(first[c][-1], *step[c][0]))
    chains = {}
    for g in range(2):
        for c in "ab":
            chains[c, g] = [jnp.concatenate(first[c][2 * g:2 * g + 2], axis=0)]
    for k in range(3):
        for g in range(2):
            for c in "ab":
                chains[c, g].append(hop(chains[c, g][-1], *step[c][1]))

    me = lax.axis_index("zero")
    sign = 1 - 2 * (lax.axis_index("bank") % 2)
    y, x = me // COLS, me % COLS

    def device(c, j, k):
        (ay, ax), (by, bx) = step[c]
        dy, dx = j * ay + k * by, j * ax + k * bx
        return ((y - sign * dy) % ROWS) * COLS + (x - sign * dx) % COLS

    at, early, late = [], [], {0: [], 1: []}
    for c in "ab":
        for j in range(4):
            at.append(device(c, j, 0))
            early.append((first[c][j], [(0 if c == "a" else 2, len(at) - 1)]))
        for g in range(2):
            for k in range(1, 4):
                pieces = []
                for j in (2 * g, 2 * g + 1):
                    at.append(device(c, j, k))
                    pieces.append((0 if c == "a" else 2, len(at) - 1))
                (late[g] if k == 3 else early).append((chains[c, g][k], pieces))
    at = jnp.stack(at).astype(jnp.int32)
    final = place(at, early)
    final = place(at, late[0], final)
    final = place(at, late[1], final)

    row, _ = lax.optimization_barrier((row, chains["a", 0][1]))
    serve = from_everyone(row, "bank").reshape(64, 2048).T
    return final, scale_down, serve


def solution(mesh):
    return jax.shard_map(
        shards,
        mesh=mesh,
        in_specs=(P("bank", None, "zero"), P("bank", None, "zero"), P("zero", "bank"), P("zero")),
        out_specs=(P("bank", None, None), P("bank", None), P()),
        check_vma=False,
    )
```

```python
import functools

import jax
import jax.numpy as jnp
from jax import lax
from jax.experimental import pallas as pl
from jax.experimental.pallas import tpu as pltpu
from jax.sharding import PartitionSpec as P

BANKS, ROWS, COLS = 16, 4, 4


def pairs(dy, dx):
    out = []
    for bank in range(BANKS):
        sign = 1 if bank % 2 == 0 else -1
        for y in range(ROWS):
            for x in range(COLS):
                to = ((y + sign * dy) % ROWS) * COLS + (x + sign * dx) % COLS
                out.append((bank * 16 + y * COLS + x, bank * 16 + to))
    return out


def hop(value, dy, dx):
    return lax.ppermute(value, ("bank", "zero"), pairs(dy, dx))


def from_everyone(value, axis):
    count = lax.axis_size(axis)
    return lax.all_to_all(jnp.broadcast_to(value[None], (count, *value.shape)), axis, 0, 0, tiled=True)


def place(at, blocks, out=None):
    arrays = [array for array, _ in blocks]
    n = sum(len(pieces) for _, pieces in blocks)

    def body(at_ref, *refs):
        out_ref, sems = refs[-2], refs[-1]
        copies = []
        for ref, (_, pieces) in zip(refs, blocks):
            for j, (expert, i) in enumerate(pieces):
                target = out_ref.at[pl.ds(expert, 2), :, pl.ds(pl.multiple_of(at_ref[i] * 128, 128), 128)]
                copies.append(pltpu.make_async_copy(ref.at[pl.ds(2 * j, 2)], target, sems.at[len(copies)]))
        for copy in copies:
            copy.start()
        for copy in copies:
            copy.wait()

    specs = [pl.BlockSpec(memory_space=pltpu.SMEM)] + [pl.BlockSpec(memory_space=pltpu.VMEM)] * len(arrays)
    args = [at] + arrays
    aliases = {}
    if out is not None:
        aliases = {len(args): 0}
        specs.append(pl.BlockSpec(memory_space=pl.ANY))
        args.append(out)
    return pl.pallas_call(
        body,
        out_shape=jax.ShapeDtypeStruct((4, 1024, 2048), jnp.bfloat16),
        in_specs=specs,
        out_specs=pl.BlockSpec(memory_space=pl.ANY),
        scratch_shapes=[pltpu.SemaphoreType.DMA((n,))],
        input_output_aliases=aliases,
        compiler_params=pltpu.CompilerParams(vmem_limit_bytes=9 << 20),
    )(*args)


def shards(master_down, second_down, router_weight, router_gain):
    merged = master_down + second_down.astype(jnp.float32)
    local = jnp.max(jnp.abs(merged), axis=2)
    local, router_weight, router_gain = lax.optimization_barrier((local, router_weight, router_gain))
    part = (router_weight * router_gain[:, None]).T
    seen = from_everyone(jnp.concatenate([local, part], axis=1), "zero")
    scale_down = jnp.max(seen[:, :, :1024], axis=0)
    row = jnp.moveaxis(seen[:, :, 1024:], 0, 1).reshape(4, 2048).astype(jnp.bfloat16)
    narrow = (merged / jnp.expand_dims(scale_down, 2)).astype(jnp.bfloat16)

    step = {"a": ((0, 1), (1, 0)), "b": ((1, 0), (0, 1))}
    me = lax.axis_index("zero")
    sign = 1 - 2 * (lax.axis_index("bank") % 2)
    y, x = me // COLS, me % COLS
    at = []

    def pieces(c, g, k):
        (ay, ax), (by, bx) = step[c]
        out = []
        for j in (2 * g, 2 * g + 1):
            dy, dx = j * ay + k * by, j * ax + k * bx
            at.append(((y - sign * dy) % ROWS) * COLS + (x - sign * dx) % COLS)
            out.append((0 if c == "a" else 2, len(at) - 1))
        return out

    where = {(c, g, k): pieces(c, g, k) for c in "ab" for g in range(2) for k in range(4)}
    at = jnp.stack(at).astype(jnp.int32)

    first = {"a": [narrow[:2]], "b": [narrow[2:]]}
    for k in range(3):
        for c in "ab":
            first[c].append(hop(first[c][-1], *step[c][0]))
    here = {}
    for g in range(2):
        for c in "ab":
            here[c, g, 0] = jnp.concatenate(first[c][2 * g:2 * g + 2], axis=0)

    def put(keys, out):
        return place(at, [(here[key], where[key]) for key in keys], out)

    def move(g, k):
        for c in "ab":
            here[c, g, k] = hop(here[c, g, k - 1], *step[c][1])

    def after(g, k, *values):
        here["a", g, k], here["b", g, k], *values = lax.optimization_barrier((here["a", g, k], here["b", g, k], *values))
        return values

    move(0, 1)
    move(1, 1)
    final = put([(c, g, 0) for c in "ab" for g in range(2)], None)
    final, row = after(0, 1, final, row)
    serve = from_everyone(row, "bank")
    move(0, 2)
    move(1, 2)
    final = put([(c, g, 1) for c in "ab" for g in range(2)], final)
    serve = serve.reshape(64, 2048)
    final, serve = after(0, 2, final, serve)
    move(0, 3)
    move(1, 3)
    final = put([(c, g, 2) for c in "ab" for g in range(2)], final)
    final = put([(c, 0, 3) for c in "ab"], final)
    final = put([(c, 1, 3) for c in "ab"], final)
    return final, scale_down, serve.T


def solution(mesh):
    return jax.shard_map(
        shards,
        mesh=mesh,
        in_specs=(P("bank", None, "zero"), P("bank", None, "zero"), P("zero", "bank"), P("zero")),
        out_specs=(P("bank", None, None), P("bank", None), P()),
        check_vma=False,
    )
```

```python
import jax
import jax.numpy as jnp
from jax import lax
from jax.experimental import pallas as pl
from jax.experimental.pallas import tpu as pltpu
from jax.sharding import PartitionSpec as P


LIMIT = 9
BANKS, ROWS, COLS = 16, 4, 4


def pairs(dy, dx):
    out = []
    for bank in range(BANKS):
        sign = 1 if bank % 2 == 0 else -1
        for y in range(ROWS):
            for x in range(COLS):
                to = ((y + sign * dy) % ROWS) * COLS + (x + sign * dx) % COLS
                out.append((bank * 16 + y * COLS + x, bank * 16 + to))
    return out


def hop(value, dy, dx):
    return lax.ppermute(value, ("bank", "zero"), pairs(dy, dx))


def from_everyone(value, axis):
    count = lax.axis_size(axis)
    return lax.all_to_all(jnp.broadcast_to(value[None], (count, *value.shape)), axis, 0, 0, tiled=True)


def swap(value, bit):
    other = lax.ppermute(value, "bank", [(bank, bank ^ bit) for bank in range(BANKS)])
    upper = (lax.axis_index("bank") & bit) != 0
    return jnp.where(upper, jnp.concatenate([other, value]), jnp.concatenate([value, other]))


def place(at, blocks, out=None):
    arrays = [array for array, _ in blocks]
    n = sum(len(pieces) for _, pieces in blocks)

    def body(at_ref, *refs):
        out_ref, sems = refs[-2], refs[-1]
        copies = []
        for ref, (_, pieces) in zip(refs, blocks):
            for j, (expert, i) in enumerate(pieces):
                target = out_ref.at[pl.ds(expert, 2), :, pl.ds(pl.multiple_of(at_ref[i] * 128, 128), 128)]
                copies.append(pltpu.make_async_copy(ref.at[pl.ds(2 * j, 2)], target, sems.at[len(copies)]))
        for copy in copies:
            copy.start()
        for copy in copies:
            copy.wait()

    specs = [pl.BlockSpec(memory_space=pltpu.SMEM)] + [pl.BlockSpec(memory_space=pltpu.VMEM)] * len(arrays)
    args = [at] + arrays
    aliases = {}
    if out is not None:
        aliases = {len(args): 0}
        specs.append(pl.BlockSpec(memory_space=pl.ANY))
        args.append(out)
    return pl.pallas_call(
        body,
        out_shape=jax.ShapeDtypeStruct((4, 1024, 2048), jnp.bfloat16),
        in_specs=specs,
        out_specs=pl.BlockSpec(memory_space=pl.ANY),
        scratch_shapes=[pltpu.SemaphoreType.DMA((n,))],
        input_output_aliases=aliases,
        compiler_params=pltpu.CompilerParams(vmem_limit_bytes=LIMIT << 20),
    )(*args)


def shards(master_down, second_down, router_weight, router_gain):
    merged = master_down + second_down.astype(jnp.float32)
    local = jnp.max(jnp.abs(merged), axis=2)
    local, router_weight, router_gain = lax.optimization_barrier((local, router_weight, router_gain))
    part = (router_weight * router_gain[:, None]).T
    seen = from_everyone(jnp.concatenate([local, part], axis=1), "zero")
    scale_down = jnp.max(seen[:, :, :1024], axis=0)
    row = jnp.moveaxis(seen[:, :, 1024:], 0, 1).reshape(4, 2048).astype(jnp.bfloat16)
    narrow = (merged / jnp.expand_dims(scale_down, 2)).astype(jnp.bfloat16)

    axes = {"a": ((0, 1), (1, 0)), "b": ((1, 0), (0, 1))}
    me = lax.axis_index("zero")
    sign = 1 - 2 * (lax.axis_index("bank") % 2)
    y, x = me // COLS, me % COLS
    groups = {"o": (0,), "g": (1, 2), "t": (3,)}
    at, where = [], {}
    for c in "ab":
        (ay, ax), (by, bx) = axes[c]
        for name, members in groups.items():
            for k in range(4):
                where[c, name, k] = []
                for j in members:
                    dy, dx = j * ay + k * by, j * ax + k * bx
                    where[c, name, k].append((0 if c == "a" else 2, len(at)))
                    at.append(((y - sign * dy) % ROWS) * COLS + (x - sign * dx) % COLS)
    at = jnp.stack(at).astype(jnp.int32)

    here = {("a", "o", 0): narrow[:2], ("b", "o", 0): narrow[2:]}
    line = {"a": [narrow[:2]], "b": [narrow[2:]]}

    def put(out, *keys):
        return place(at, [(here[c, *key], where[c, *key]) for key in keys for c in "ab"], out)

    def along():
        for c in "ab":
            line[c].append(hop(line[c][-1], *axes[c][0]))

    def across(name, k):
        for c in "ab":
            here[c, name, k] = hop(here[c, name, k - 1], *axes[c][1])

    def after(name, k, *values):
        one, two, *values = lax.optimization_barrier((here["a", name, k], here["b", name, k], *values))
        here["a", name, k], here["b", name, k] = one, two
        return values if len(values) > 1 else values[0]

    along()
    across("o", 1)
    row = swap(row, 1)
    along()
    across("o", 2)
    row = swap(row, 2)
    along()
    for c in "ab":
        here[c, "g", 0] = jnp.concatenate(line[c][1:3], axis=0)
        here[c, "t", 0] = line[c][3]
    across("g", 1)
    across("o", 3)
    across("t", 1)
    final = put(None, ("o", 0), ("o", 1))
    final = put(final, ("o", 2), ("g", 0))
    final = after("g", 1, final)
    across("g", 2)
    row = swap(row, 4)
    final = put(final, ("o", 3), ("t", 0))
    final = put(final, ("g", 1))
    final = after("t", 1, final)
    across("t", 2)
    serve = swap(row, 8)
    final = put(final, ("t", 1))
    final = after("g", 2, final)
    across("g", 3)
    across("t", 3)
    final = put(final, ("g", 2), ("t", 2))
    final, serve = lax.optimization_barrier((final, serve))
    final = put(final, ("g", 3))
    final = put(final, ("t", 3))
    return final, scale_down, serve.T


def solution(mesh):
    return jax.shard_map(
        shards,
        mesh=mesh,
        in_specs=(P("bank", None, "zero"), P("bank", None, "zero"), P("zero", "bank"), P("zero")),
        out_specs=(P("bank", None, None), P("bank", None), P()),
        check_vma=False,
    )
```
